32 devices in a mesh: dp: 4 (over y, z), ctx: 8 (over x, core).
Axes of the slice: x: 4, y: 2, z: 2, core: 2. Of those that a mesh axis runs over, the one named last changes fastest.
The devices are a block of a 4x4x8 slice.
Arguments:
- hidden: bfloat16 [1024, 2048], P(('dp', 'ctx')), parts along dimension 0
- w_q: bfloat16 [2048, 3072], replicated
- w_uk: bfloat16 [16, 128, 512], replicated
- w_uv: bfloat16 [16, 512, 128], replicated
- w_o: bfloat16 [2048, 2048], replicated
- kv_prefix: bfloat16 [65536, 576], P(('dp', 'ctx')), parts along dimension 0
- kv_suffix: bfloat16 [1024, 1024, 576], P(('dp', 'ctx')), parts along dimension 0
- seq_lens: int32 [1024], P(('dp', 'ctx')), parts along dimension 0
Outputs:
- output: bfloat16 [1024, 2048], P(('dp', 'ctx')), parts along dimension 0
There are 4 independent parts. The reference program is written for one: setup_inputs(seed, part) draws one part's arguments, and reference() takes and returns one part's arrays. A program takes and returns all parts, laid end to end along the dimension named above; an argument that names none is the same for every part.
All inputs are finite; a program needn't handle non-finite values.
Results may differ from the reference program's by a relative error of at most 0.00660993.
Values are sent between devices in bfloat16 or wider.
A program may use at most 768 MiB of HBM per device.

```python
import math
import jax
import jax.numpy as jnp
from jax import lax

MODEL_DIM = 2048
HEADS = 16
NOPE_DIM = 128
ROPE_DIM = 64
VALUE_DIM = 128
LATENT_DIM = 512
GROUP_SIZE = 8
SEQUENCES = 256
PREFIX_LEN = 16384
SUFFIX_LEN = 1024
ROPE_BASE = 10000

KV_WIDTH = LATENT_DIM + ROPE_DIM
QK_WIDTH = NOPE_DIM + ROPE_DIM
SCORE_SCALE = QK_WIDTH ** -0.5
BLOCK_LEN = PREFIX_LEN // GROUP_SIZE
PREFIX_AMP = 1.5
SUFFIX_AMP = PREFIX_AMP * math.sqrt(1.0 + 2.0 * math.log(max(2.0 * PREFIX_LEN / SUFFIX_LEN, 1.0)) * QK_WIDTH / (PREFIX_AMP ** 2 * LATENT_DIM))


def draw_lengths(key):
    raw_lens = jax.random.randint(key, (SEQUENCES,), 0, SUFFIX_LEN, jnp.int32)
    seq_index = jnp.arange(SEQUENCES)
    return jnp.where(seq_index == 0, SUFFIX_LEN - 1, jnp.where(seq_index == 1, 0, raw_lens)).astype(jnp.int32)


def latent_cache(noise, means):
    rope_pad = jnp.zeros(means.shape[:-1] + (ROPE_DIM,), jnp.float32)
    return noise + jnp.concatenate([means, rope_pad], axis=-1)


def setup_inputs(seed: int = 0, part: int = 0) -> dict:
    shared_keys = jax.random.split(jax.random.key(seed + 1), 4)
    own_keys = jax.random.split(jax.random.fold_in(jax.random.key(seed), part), 6)
    hidden = jax.random.normal(own_keys[0], (SEQUENCES, MODEL_DIM), jnp.float32)
    w_q = jax.random.normal(shared_keys[0], (MODEL_DIM, HEADS * QK_WIDTH), jnp.float32) * MODEL_DIM ** -0.5
    w_uk = jax.random.normal(shared_keys[1], (HEADS, NOPE_DIM, LATENT_DIM), jnp.float32) * NOPE_DIM ** -0.5
    w_uv = jax.random.normal(shared_keys[2], (HEADS, LATENT_DIM, VALUE_DIM), jnp.float32) * LATENT_DIM ** -0.5
    w_o = jax.random.normal(shared_keys[3], (HEADS * VALUE_DIM, MODEL_DIM), jnp.float32) * (HEADS * VALUE_DIM) ** -0.5
    pre_noise = jax.random.normal(own_keys[1], (GROUP_SIZE, BLOCK_LEN, KV_WIDTH), jnp.float32)
    pre_means = jax.random.normal(own_keys[2], (GROUP_SIZE, 1, LATENT_DIM), jnp.float32) * PREFIX_AMP
    kv_prefix = latent_cache(pre_noise, pre_means).reshape(PREFIX_LEN, KV_WIDTH)
    suf_noise = jax.random.normal(own_keys[3], (SEQUENCES, SUFFIX_LEN, KV_WIDTH), jnp.float32)
    suf_means = jax.random.normal(own_keys[4], (SEQUENCES, 1, LATENT_DIM), jnp.float32) * SUFFIX_AMP
    kv_suffix = latent_cache(suf_noise, suf_means)
    seq_lens = draw_lengths(own_keys[5])
    return {'hidden': hidden.astype(jnp.bfloat16), 'w_q': w_q.astype(jnp.bfloat16), 'w_uk': w_uk.astype(jnp.bfloat16), 'w_uv': w_uv.astype(jnp.bfloat16), 'w_o': w_o.astype(jnp.bfloat16), 'kv_prefix': kv_prefix.astype(jnp.bfloat16), 'kv_suffix': kv_suffix.astype(jnp.bfloat16), 'seq_lens': seq_lens}


def rope_rotate(rot_in, positions):
    half_dim = ROPE_DIM // 2
    inv_freq = jnp.exp(jnp.arange(half_dim, dtype=jnp.float32) * (-math.log(ROPE_BASE) / half_dim))
    angle = positions.astype(jnp.float32)[:, None, None] * inv_freq
    cos_part = jnp.cos(angle)
    sin_part = jnp.sin(angle)
    rot_wide = rot_in.astype(jnp.float32)
    first_half = rot_wide[..., :half_dim]
    second_half = rot_wide[..., half_dim:]
    return jnp.concatenate([first_half * cos_part - second_half * sin_part, second_half * cos_part + first_half * sin_part], axis=-1)


def reference(hidden, w_q, w_uk, w_uv, w_o, kv_prefix, kv_suffix, seq_lens):
    q_all = jnp.dot(hidden, w_q, preferred_element_type=jnp.float32).astype(jnp.bfloat16).reshape(SEQUENCES, HEADS, QK_WIDTH)
    q_lat = jnp.einsum('bhn,hnc->bhc', q_all[..., :NOPE_DIM].astype(jnp.float32), w_uk.astype(jnp.float32)).astype(jnp.bfloat16)
    q_rot = rope_rotate(q_all[..., NOPE_DIM:], PREFIX_LEN + seq_lens).astype(jnp.bfloat16)
    query = jnp.concatenate([q_lat, q_rot], axis=-1)
    pre_keys = kv_prefix.astype(jnp.float32)
    pre_vals = pre_keys[:, :LATENT_DIM]
    slots = jnp.arange(SUFFIX_LEN)

    def one_sequence(item):
        q_row, suf_row, length = item
        q_row = q_row.astype(jnp.float32)
        suf_keys = suf_row.astype(jnp.float32)
        s_pre = jnp.einsum('hw,pw->hp', q_row, pre_keys) * SCORE_SCALE
        s_suf = jnp.einsum('hw,sw->hs', q_row, suf_keys) * SCORE_SCALE
        s_suf = jnp.where((slots <= length)[None, :], s_suf, -jnp.inf)
        probs = jax.nn.softmax(jnp.concatenate([s_pre, s_suf], axis=-1), axis=-1)
        return jnp.dot(probs[:, :PREFIX_LEN], pre_vals) + jnp.dot(probs[:, PREFIX_LEN:], suf_keys[:, :LATENT_DIM])

    o_lat = lax.map(one_sequence, (query, kv_suffix, seq_lens)).astype(jnp.bfloat16)
    o_val = jnp.einsum('bhc,hcv->bhv', o_lat.astype(jnp.float32), w_uv.astype(jnp.float32)).astype(jnp.bfloat16)
    out = hidden.astype(jnp.float32) + jnp.dot(o_val.reshape(SEQUENCES, HEADS * VALUE_DIM), w_o, preferred_element_type=jnp.float32)
    return out.astype(jnp.bfloat16)
```

```python
import functools
import math
import jax
import jax.numpy as jnp
from jax import lax
from jax.experimental import pallas as pl
from jax.experimental.pallas import tpu as pltpu
from jax.sharding import PartitionSpec as P

ROPE_BASE = 10000
CORES = 2
LOG2E = math.log2(math.e)
CHUNK = 1024
SLOTS = 256
LANES = 128
UNROLL = 2
VMEM_LIMIT = 64_000_000
F32 = jnp.float32
BF16 = jnp.bfloat16
NT = (((1,), (1,)), ((), ()))


def dot(a, b):
    return jnp.dot(a, b, preferred_element_type=F32)


def dot_nt(a, b):
    return lax.dot_general(a, b, NT, preferred_element_type=F32)


def split_dot(wide, w):
    rows = wide.shape[0]
    upper = wide.astype(BF16)
    lower = (wide - upper.astype(F32)).astype(BF16)
    both = dot(jnp.concatenate([upper, lower], axis=0), w)
    return both[:rows] + both[rows:]


def prefix_kernel(chips, scale, hidden, trig, w_q, w_uk, w_uv, kv, q_own, part,
                  hid_all, trig_all, wq_v, wuk_v, wuv_v, keys, q_blk, acc, vbuf,
                  w_sem, key_sem, h_send, h_recv, q_send, q_recv, p_send, p_recv, own_sem):
    me = lax.axis_index('ctx')
    n = chips * CORES
    chip = me // CORES
    par = me % CORES
    rows = hidden.shape[0]
    block = kv.shape[0]
    lat = w_uk.shape[2]
    nope = w_uk.shape[1]
    heads = wuk_v.shape[0]
    rot = kv.shape[1] - lat
    width = wq_v.shape[1]
    seqs = CORES * rows
    mine = pl.ds(pl.multiple_of(par * rows, rows), rows)
    other = pl.ds(pl.multiple_of((1 - par) * rows, rows), rows)
    partner = chip * CORES + (1 - par)

    def remote(src, dst, send, recv, dev):
        return pltpu.make_async_remote_copy(src_ref=src, dst_ref=dst, send_sem=send, recv_sem=recv,
                                            device_id={'ctx': dev}, device_id_type=pl.DeviceIdType.MESH)

    load_wq = pltpu.make_async_copy(w_q.at[:, pl.ds(pl.multiple_of(par * width, width), width)], wq_v, w_sem.at[0])
    load_wuk = pltpu.make_async_copy(w_uk.at[pl.ds(par * heads, heads)], wuk_v, w_sem.at[1])
    load_wuv = pltpu.make_async_copy(w_uv.at[pl.ds(par * heads, heads)], wuv_v, w_sem.at[2])
    load_keys = pltpu.make_async_copy(kv, keys.at[pl.ds(0, block)], w_sem.at[3])
    load_wq.start()
    load_wuk.start()
    load_keys.start()
    load_wuv.start()

    barrier = pltpu.get_barrier_semaphore()
    for k in range(1, n):
        pl.semaphore_signal(barrier, inc=1, device_id={'ctx': (me + k) % n}, device_id_type=pl.DeviceIdType.MESH)
    pl.semaphore_wait(barrier, n - 1)

    def direct(d):
        dev = partner if d == 0 else ((chip + d) % chips) * CORES + par
        slot = 0 if d == 0 else chips - d
        return (remote(hidden, hid_all.at[chip, mine], h_send.at[0, d], h_recv.at[0, slot], dev),
                remote(trig, trig_all.at[chip, mine], h_send.at[1, d], h_recv.at[1, slot], dev))

    def relay(off):
        c = (chip + off) % chips
        return (remote(hid_all.at[c, mine], hid_all.at[c, mine], h_send.at[0, chips + off], h_recv.at[0, chips + off], partner),
                remote(trig_all.at[c, mine], trig_all.at[c, mine], h_send.at[1, chips + off], h_recv.at[1, chips + off], partner))

    def arrival(slot, off, where):
        c = (chip + off) % chips
        return (remote(hid_all.at[c, where], hid_all.at[c, where], h_send.at[0, 0], h_recv.at[0, slot], partner),
                remote(trig_all.at[c, where], trig_all.at[c, where], h_send.at[1, 0], h_recv.at[1, slot], partner))

    def swap_keys():
        return remote(kv, keys.at[pl.ds(block, block)], key_sem.at[0], key_sem.at[1], partner)

    order = [0, 1, chips - 1] + list(range(2, chips - 1))
    for d in order:
        for copy in direct(d):
            copy.start()
    swap_keys().start()
    hid_all[chip, mine, :] = hidden[...]
    trig_all[chip, mine, :] = trig[...]
    load_wq.wait()
    load_wuk.wait()
    for copy in arrival(0, 0, other):
        copy.wait_recv()

    lane = lax.broadcasted_iota(jnp.int32, (seqs, 2 * rot), 1)
    c2 = scale * LOG2E

    def project(off):
        c = (chip + off) % chips
        q_all = dot(hid_all[c], wq_v[...]).astype(BF16).astype(F32)
        tri = trig_all[c]
        tri_r = pltpu.roll(tri, rot, 1)
        cos_t = jnp.where(lane < rot, tri, tri_r)
        sin_t = jnp.where(lane < rot, tri_r, tri)
        for i in range(heads // 2):
            base = i * 2 * (nope + rot)
            even = q_all[:, base:base + nope]
            rest = pltpu.roll(q_all[:, base + nope:base + 2 * (nope + rot)], 2 * nope - rot, 1)
            odd = rest[:, :nope]
            pe = rest[:, nope:]
            half = rot // 2
            swapped = jnp.where(lane % rot < half, pltpu.roll(pe, 2 * rot - half, 1), pltpu.roll(pe, half, 1))
            pe = pe * cos_t + swapped * sin_t
            q_blk[2 * i, :, :lat] = dot(even.astype(BF16), wuk_v[2 * i]).astype(BF16)
            q_blk[2 * i + 1, :, :lat] = dot(odd.astype(BF16), wuk_v[2 * i + 1]).astype(BF16)
            q_blk[2 * i + 1, :, lat:] = pe[:, :rot].astype(BF16)
            q_blk[2 * i, :, lat:] = pltpu.roll(pe, rot, 1)[:, :rot].astype(BF16)

    def own_queries():
        return (pltpu.make_async_copy(q_blk.at[:, mine], q_own.at[par], own_sem.at[0]),
                remote(q_blk.at[:, other], q_own.at[par], q_send, q_recv, partner))

    def own_part():
        return (pltpu.make_async_copy(vbuf.at[0, :, mine], part.at[chip, par], own_sem.at[1]),
                remote(vbuf.at[0, :, other], part.at[chip, par], p_send.at[0, 1], p_recv.at[chip, par], partner))

    def far_part(off):
        c = (chip + off) % chips
        return (remote(vbuf.at[off, :, mine], part.at[chip, par], p_send.at[off, 0], p_recv.at[chip, par], c * CORES + par),
                remote(vbuf.at[off, :, other], part.at[chip, par], p_send.at[off, 1], p_recv.at[chip, par], c * CORES + (1 - par)))

    def attend(off, state, start):
        m, l = state
        q = q_blk[...].reshape(heads * seqs, lat + rot)
        for j in range(block // CHUNK):
            k_c = keys[pl.ds(start + j * CHUNK, CHUNK), :]
            s = dot_nt(q, k_c)
            top = jnp.max(s, axis=1, keepdims=True)
            m_new = top if m is None else jnp.maximum(m, top)
            p = jnp.exp2((s - m_new) * c2)
            total = jnp.sum(p, axis=1, keepdims=True)
            o = dot(p.astype(BF16), k_c[:, :lat])
            if m is None:
                l = total
                acc[...] = o
            else:
                fade = jnp.exp2((m - m_new) * c2)
                l = l * fade + total
                acc[...] = acc[...] * fade + o
            m = m_new
        return m, l

    def body(off, carry):
        @pl.when(off > 0)
        def _():
            for copy in arrival(chips + off, off, other):
                copy.wait_recv()
        project(off)

        @pl.when(off == 0)
        def _():
            for copy in own_queries():
                copy.start()
            load_keys.wait()
        state = attend(off, (None, None), 0)

        @pl.when(off == 0)
        def _():
            swap_keys().wait_recv()

        @pl.when(off < chips - 1)
        def _():
            nxt = off + 1
            for copy in arrival(nxt, nxt, mine):
                copy.wait_recv()
            for copy in relay(nxt):
                copy.start()
        m, l = attend(off, state, block)

        @pl.when(off == 0)
        def _():
            load_wuv.wait()
        inv = 1.0 / l
        lse = m * scale + jnp.log(l)
        lanes = lax.broadcasted_iota(jnp.int32, (seqs, vbuf.shape[-1]), 1)
        tile = jnp.zeros((seqs, vbuf.shape[-1]), F32)
        for h in range(heads):
            at = slice(h * seqs, (h + 1) * seqs)
            vbuf[off, h] = split_dot(acc[at, :] * inv[at], wuv_v[h])
            tile = jnp.where(lanes == h, lse[at], tile)
        vbuf[off, heads] = tile

        @pl.when(off == 0)
        def _():
            for copy in own_part():
                copy.start()
            for copy in own_queries():
                copy.wait()

        @pl.when(off > 0)
        def _():
            for copy in far_part(off):
                copy.start()
        return carry

    lax.fori_loop(0, chips, body, 0)

    for d in range(chips):
        for copy in direct(d):
            copy.wait_send()
    swap_keys().wait_send()
    for off in range(1, chips):
        for copy in relay(off):
            copy.wait_send()
        for copy in far_part(off):
            copy.wait_send()
    local, near = own_part()
    local.wait()
    near.wait_send()
    for off in range(chips):
        c = (chip + off) % chips
        for k, who in enumerate((par, 1 - par)):
            if off == 0 and k == 0:
                continue
            remote(vbuf.at[0, :, mine], part.at[c, who], p_send.at[0, 0], p_recv.at[c, who], partner).wait_recv()


def suffix_kernel(chips, scale, lens, q, hidden, part, w_uv, w_o, kv, out,
                  keys, s_all, o_seq, o_all, part_v, wuv_v, wo_v, v_all, todo, key_sem, w_sem):
    rows = hidden.shape[0]
    heads, lat = w_uv.shape[0], w_uv.shape[1]
    vdim = w_uv.shape[2]
    per = kv.shape[1] // SLOTS
    c2 = scale * LOG2E

    def load(idx):
        b, k = idx // per, idx % per
        return pltpu.make_async_copy(kv.at[b, pl.ds(pl.multiple_of(k * SLOTS, SLOTS), SLOTS)], keys.at[idx], key_sem.at[idx])

    def plan(b, count):
        def one(k, count):
            todo[count] = b * per + k
            load(b * per + k).start()
            return count + 1
        return lax.fori_loop(0, lens[b] // SLOTS + 1, one, count)

    total = lax.fori_loop(0, rows, plan, 0)
    for u in range(UNROLL - 1):
        todo[total + u] = todo[total - 1]
    loads = (pltpu.make_async_copy(part, part_v, w_sem.at[0]),
             pltpu.make_async_copy(w_uv, wuv_v, w_sem.at[1]),
             pltpu.make_async_copy(w_o, wo_v, w_sem.at[2]))
    for copy in loads:
        copy.start()
    s_all[...] = jnp.full(s_all.shape, -jnp.inf, F32)
    o_seq[...] = jnp.zeros(o_seq.shape, F32)
    steps = (total + UNROLL - 1) // UNROLL
    lane = lax.broadcasted_iota(jnp.int32, (heads, SLOTS), 1)

    def score(i, carry):
        ids = [todo[i * UNROLL + u] for u in range(UNROLL)]
        for u, idx in enumerate(ids):
            @pl.when(i * UNROLL + u < total)
            def _():
                load(idx).wait()
        vals = [dot_nt(q[idx // per], keys[idx]) for idx in ids]
        for idx, val in zip(ids, vals):
            b, k = idx // per, idx % per
            val = jnp.where(lane <= lens[b] - k * SLOTS, val, -jnp.inf)
            for t in range(SLOTS // LANES):
                s_all[k * (SLOTS // LANES) + t, pl.ds(b, heads, stride=rows), :] = val[:, t * LANES:(t + 1) * LANES]
        return carry

    lax.fori_loop(0, steps, score, 0)

    ms, ls = [], []
    for h in range(heads):
        at = slice(h * rows, (h + 1) * rows)
        s = s_all[:, at, :]
        m = jnp.max(jnp.max(s, axis=0), axis=1, keepdims=True)
        p = jnp.exp2((s - m) * c2)
        ms.append(m)
        ls.append(jnp.sum(jnp.sum(p, axis=0), axis=1, keepdims=True))
        s_all[:, at, :] = p

    def gather(i, carry):
        ids = [todo[i * UNROLL + u] for u in range(UNROLL)]
        vals = []
        for idx in ids:
            b, k = idx // per, idx % per
            p = jnp.concatenate([s_all[k * (SLOTS // LANES) + t, pl.ds(b, heads, stride=rows), :] for t in range(SLOTS // LANES)], axis=1)
            vals.append(dot(p.astype(BF16), keys[idx, :, :lat]))
        for u, (idx, val) in enumerate(zip(ids, vals)):
            to = jnp.where(i * UNROLL + u < total, idx // per, rows)
            o_seq[to] += val
        return carry

    lax.fori_loop(0, steps, gather, 0)
    for b in range(rows):
        for t in range(lat // LANES):
            o_all[t, pl.ds(b, heads, stride=rows), :] = o_seq[b, :, t * LANES:(t + 1) * LANES]
    for copy in loads:
        copy.wait()
    half = heads // CORES
    for h in range(heads):
        at = slice(h * rows, (h + 1) * rows)
        side, i = h // half, h % half
        o = jnp.concatenate([o_all[t, at, :] for t in range(lat // LANES)], axis=1) / ls[h]
        v_suf = split_dot(o, wuv_v[h])
        lse = ms[h] * scale + jnp.log(ls[h])
        far = [part_v[c, side, half][:, i:i + 1] for c in range(chips)]
        top = functools.reduce(jnp.maximum, far, lse)
        w_suf = jnp.exp(lse - top)
        norm = w_suf
        v = v_suf * w_suf
        for c in range(chips):
            w_far = jnp.exp(far[c] - top)
            norm = norm + w_far
            v = v + part_v[c, side, i] * w_far
        v_all[:, h * vdim:(h + 1) * vdim] = (v / norm).astype(BF16)
    out[...] = (hidden[...].astype(F32) + dot(v_all[...], wo_v[...])).astype(BF16)


def solution(mesh):
    group = mesh.shape['ctx']
    chips = group // CORES
    rows_spec = P(('dp', 'ctx'), None)
    whole_spec = P()
    hbm = pl.BlockSpec(memory_space=pl.ANY)
    vmem = pl.BlockSpec(memory_space=pltpu.VMEM)
    smem = pl.BlockSpec(memory_space=pltpu.SMEM)

    def local_step(hidden, w_q, w_uk, w_uv, w_o, kv_prefix, kv_suffix, seq_lens):
        rows, dim = hidden.shape
        heads, nope, lat = w_uk.shape
        vdim = w_uv.shape[2]
        block, kv_width = kv_prefix.shape
        rot = kv_width - lat
        slots = kv_suffix.shape[1]
        scale = (w_q.shape[1] // heads) ** -0.5
        half = heads // CORES
        seqs = CORES * rows

        inv_freq = jnp.exp(jnp.arange(rot // 2, dtype=F32) * (-math.log(ROPE_BASE) / (rot // 2)))
        angle = (block * group + seq_lens).astype(F32)[:, None] * inv_freq
        cos_part, sin_part = jnp.cos(angle), jnp.sin(angle)
        trig = jnp.concatenate([cos_part, cos_part, -sin_part, sin_part], axis=1)

        q_own, part = pl.pallas_call(
            functools.partial(prefix_kernel, chips, scale),
            name='prefix',
            out_shape=(jax.ShapeDtypeStruct((CORES, half, rows, kv_width), BF16),
                       jax.ShapeDtypeStruct((chips, CORES, half + 1, rows, vdim), F32)),
            in_specs=[vmem, vmem, hbm, hbm, hbm, hbm],
            out_specs=(hbm, hbm),
            scratch_shapes=[
                pltpu.VMEM((chips, seqs, dim), BF16),
                pltpu.VMEM((chips, seqs, 2 * rot), F32),
                pltpu.VMEM((dim, w_q.shape[1] // CORES), BF16),
                pltpu.VMEM((half, nope, lat), BF16),
                pltpu.VMEM((half, lat, vdim), BF16),
                pltpu.VMEM((CORES * block, kv_width), BF16),
                pltpu.VMEM((half, seqs, kv_width), BF16),
                pltpu.VMEM((half * seqs, lat), F32),
                pltpu.VMEM((chips, half + 1, seqs, vdim), F32),
                pltpu.SemaphoreType.DMA((4,)),
                pltpu.SemaphoreType.DMA((2,)),
                pltpu.SemaphoreType.DMA((2, 2 * chips)),
                pltpu.SemaphoreType.DMA((2, 2 * chips)),
                pltpu.SemaphoreType.DMA,
                pltpu.SemaphoreType.DMA,
                pltpu.SemaphoreType.DMA((chips, CORES)),
                pltpu.SemaphoreType.DMA((chips, CORES)),
                pltpu.SemaphoreType.DMA((2,)),
            ],
            compiler_params=pltpu.CompilerParams(collective_id=0, has_side_effects=True, vmem_limit_bytes=VMEM_LIMIT),
        )(hidden, trig, w_q, w_uk, w_uv, kv_prefix)

        q_seq = q_own.reshape(heads, rows, kv_width).transpose(1, 0, 2)
        blocks = rows * (slots // SLOTS)
        return pl.pallas_call(
            functools.partial(suffix_kernel, chips, scale),
            name='suffix',
            out_shape=jax.ShapeDtypeStruct((rows, dim), BF16),
            in_specs=[smem, vmem, vmem, hbm, hbm, hbm, hbm],
            out_specs=vmem,
            scratch_shapes=[
                pltpu.VMEM((blocks, SLOTS, kv_width), BF16),
                pltpu.VMEM((slots // LANES, heads * rows, LANES), F32),
                pltpu.VMEM((rows + 1, heads, lat), F32),
                pltpu.VMEM((lat // LANES, heads * rows, LANES), F32),
                pltpu.VMEM((chips, CORES, half + 1, rows, vdim), F32),
                pltpu.VMEM((heads, lat, vdim), BF16),
                pltpu.VMEM((heads * vdim, dim), BF16),
                pltpu.VMEM((rows, heads * vdim), BF16),
                pltpu.SMEM((blocks + UNROLL,), jnp.int32),
                pltpu.SemaphoreType.DMA((blocks,)),
                pltpu.SemaphoreType.DMA((3,)),
            ],
            compiler_params=pltpu.CompilerParams(vmem_limit_bytes=67_043_328),
        )(seq_lens, q_seq, hidden, part, w_uv, w_o, kv_suffix)

    return jax.shard_map(local_step, mesh=mesh, in_specs=(rows_spec, whole_spec, whole_spec, whole_spec, whole_spec, rows_spec, P(('dp', 'ctx'), None, None), P(('dp', 'ctx'))), out_specs=rows_spec, check_vma=False)
```

```python
import functools
import math
import jax
import jax.numpy as jnp
from jax import lax
from jax.experimental import pallas as pl
from jax.experimental.pallas import tpu as pltpu
from jax.sharding import PartitionSpec as P

ROPE_BASE = 10000
CORES = 2
LOG2E = math.log2(math.e)
CHUNK = 1024
PIECES = 4
SLOTS = 256
LANES = 128
UNROLL = 4
GROUP = 8
VMEM_LIMIT = 64_000_000
F32 = jnp.float32
BF16 = jnp.bfloat16
NT = (((1,), (1,)), ((), ()))


def dot(a, b):
    return jnp.dot(a, b, preferred_element_type=F32)


def dot_nt(a, b):
    return lax.dot_general(a, b, NT, preferred_element_type=F32)


def split_dot(wide, w):
    rows = wide.shape[0]
    upper = wide.astype(BF16)
    lower = (wide - upper.astype(F32)).astype(BF16)
    both = dot(jnp.concatenate([upper, lower], axis=0), w)
    return both[:rows] + both[rows:]


def rotation(lens, rows, start, rot):
    half = rot // 2
    row = lax.broadcasted_iota(jnp.int32, (rows, 2 * rot), 0)
    lane = lax.broadcasted_iota(jnp.int32, (rows, 2 * rot), 1)
    pos = jnp.zeros((rows, 2 * rot), jnp.int32)
    for b in range(rows):
        pos = jnp.where(row == b, start + lens[b], pos)
    freq = jnp.zeros((rows, 2 * rot), F32)
    for i in range(half):
        freq = jnp.where(lane % half == i, math.exp(-i * math.log(ROPE_BASE) / half), freq)
    angle = pos.astype(F32) * freq
    sin_t = jnp.sin(angle)
    return jnp.where(lane < rot, jnp.cos(angle), jnp.where(lane < rot + half, -sin_t, sin_t))


def prefix_kernel(chips, scale, lens, hidden, w_q, w_uk, w_uv, kv, q_own, part,
                  hid_all, trig_all, q_wide, q_turn, wq_v, wuk_v, wuv_v, keys, q_all, acc, acc_own, m_own, l_own, s_buf, p_buf, vbuf,
                  w_sem, key_sem, h_send, h_recv, q_send, q_recv, p_send, p_recv, own_sem):
    me = lax.axis_index('ctx')
    n = chips * CORES
    chip = me // CORES
    par = me % CORES
    rows = hidden.shape[0]
    block = kv.shape[1]
    lat = w_uk.shape[2]
    nope = w_uk.shape[1]
    heads = wuk_v.shape[0]
    rot = kv.shape[0] - lat
    width = wq_v.shape[1]
    seqs = CORES * rows
    near = (1, chips - 1)
    far = tuple(range(2, chips - 1))
    units = 2 + 1 + len(far)
    last = units - 1
    mine = pl.ds(pl.multiple_of(par * rows, rows), rows)
    other = pl.ds(pl.multiple_of((1 - par) * rows, rows), rows)
    partner = chip * CORES + (1 - par)

    def remote(src, dst, send, recv, dev):
        return pltpu.make_async_remote_copy(src_ref=src, dst_ref=dst, send_sem=send, recv_sem=recv,
                                            device_id={'ctx': dev}, device_id_type=pl.DeviceIdType.MESH)

    load_hid = pltpu.make_async_copy(hidden, hid_all.at[0, mine], own_sem.at[2])
    load_wq = pltpu.make_async_copy(w_q.at[:, pl.ds(pl.multiple_of(par * width, width), width)], wq_v, w_sem.at[0])
    load_wuk = pltpu.make_async_copy(w_uk.at[pl.ds(par * heads, heads)], wuk_v, w_sem.at[1])
    load_wuv = pltpu.make_async_copy(w_uv.at[pl.ds(par * heads, heads)], wuv_v, w_sem.at[2])
    load_keys = pltpu.make_async_copy(kv, keys.at[0], w_sem.at[3])
    load_hid.start()
    load_wq.start()
    load_wuk.start()
    load_keys.start()
    load_wuv.start()

    barrier = pltpu.get_barrier_semaphore()
    for k in range(1, n):
        pl.semaphore_signal(barrier, inc=1, device_id={'ctx': (me + k) % n}, device_id_type=pl.DeviceIdType.MESH)
    trig_all[0, mine, :] = rotation(lens, rows, n * block, rot)
    pl.semaphore_wait(barrier, n - 1)

    def both(dst, where, sems, slot, dev, src=0):
        return (remote(hid_all.at[src, mine], hid_all.at[dst, where], h_send.at[0, sems], h_recv.at[0, slot], dev),
                remote(trig_all.at[src, mine], trig_all.at[dst, where], h_send.at[1, sems], h_recv.at[1, slot], dev))

    def direct(d):
        if d == 0:
            return both(0, mine, 0, 0, partner)
        return both(chips - d, mine, d, chips - d, ((chip + d) % chips) * CORES + par)

    def relay(off):
        return both(off, mine, chips + off, chips + off, partner, src=off)

    def arrival(slot, off, where):
        return both(off, where, 0, slot, partner)

    def swap_keys():
        return remote(kv, keys.at[1], key_sem.at[0], key_sem.at[1], partner)

    load_hid.wait()
    for d in (0,) + near + far:
        for copy in direct(d):
            copy.start()
    swap_keys().start()
    vbuf[:, heads] = jnp.zeros((chips,) + vbuf.shape[2:], F32)
    load_wq.wait()
    load_wuk.wait()
    for copy in arrival(0, 0, other):
        copy.wait_recv()
    c2 = scale * LOG2E

    def project(hid, tri, put):
        lane = lax.broadcasted_iota(jnp.int32, (hid.shape[0], 2 * rot), 1)
        q_f = dot(hid, wq_v[...]).astype(BF16).astype(F32)
        tri_r = pltpu.roll(tri, rot, 1)
        cos_t = jnp.where(lane < rot, tri, tri_r)
        sin_t = jnp.where(lane < rot, tri_r, tri)
        for i in range(heads // 2):
            base = i * 2 * (nope + rot)
            even = q_f[:, base:base + nope]
            rest = pltpu.roll(q_f[:, base + nope:base + 2 * (nope + rot)], 2 * nope - rot, 1)
            odd = rest[:, :nope]
            pe = rest[:, nope:]
            half = rot // 2
            swapped = jnp.where(lane % rot < half, pltpu.roll(pe, 2 * rot - half, 1), pltpu.roll(pe, half, 1))
            pe = pe * cos_t + swapped * sin_t
            put(2 * i, dot(even.astype(BF16), wuk_v[2 * i]).astype(BF16), pltpu.roll(pe, rot, 1)[:, :rot].astype(BF16))
            put(2 * i + 1, dot(odd.astype(BF16), wuk_v[2 * i + 1]).astype(BF16), pe[:, :rot].astype(BF16))

    def project_chip(off, unit):
        def put(h, nope_part, rot_part):
            q_all[unit, h, :, :lat] = nope_part
            q_all[unit, h, :, lat:] = rot_part
        project(hid_all[off], trig_all[off], put)

    def project_near():
        def put(h, nope_part, rot_part):
            unit, group = (1, 2 * h) if h < heads // 2 else (last, 2 * h - heads)
            for k in range(2):
                q_all[unit, group + k, :, :lat] = nope_part[k * seqs:(k + 1) * seqs]
                q_all[unit, group + k, :, lat:] = rot_part[k * seqs:(k + 1) * seqs]
        project(jnp.concatenate([hid_all[d] for d in near], axis=0), jnp.concatenate([trig_all[d] for d in near], axis=0), put)

    def own_queries():
        to = q_own.at[:, pl.ds(pl.multiple_of(par * heads, heads), heads)]
        return (pltpu.make_async_copy(q_turn.at[mine], to, own_sem.at[0]),
                remote(q_turn.at[other], to, q_send, q_recv, partner))

    def turn_queries():
        total = lat + rot
        spans = [(t, min(LANES, total - t)) for t in range(0, total, LANES)]
        for t, w in spans:
            q_wide[t // LANES, :, :w] = q_all[0, :, :, t:t + w].reshape(heads * seqs, w).astype(F32)
        for b in range(seqs):
            for t, w in spans:
                q_turn[b, :, t:t + w] = q_wide[t // LANES, pl.ds(b, heads, stride=seqs), :][:, :w].astype(BF16)

    def own_part():
        return (pltpu.make_async_copy(vbuf.at[0, :, mine], part.at[chip, par], own_sem.at[1]),
                remote(vbuf.at[0, :, other], part.at[chip, par], p_send.at[0, 0, 1], p_recv.at[chip, par, 0], partner))

    def sent_part(off, lo, hi, turn):
        c = (chip + off) % chips
        span = pl.ds(lo, hi - lo)
        return tuple(remote(vbuf.at[off, span, where], part.at[chip, par, span], p_send.at[off, turn, k], p_recv.at[chip, par, turn], c * CORES + dev)
                     for k, (where, dev) in enumerate(((mine, par), (other, 1 - par))))

    def attend(unit, state, chunks, acc):
        queries = heads * seqs
        q = q_all[unit].reshape(queries, lat + rot)
        wide, tall = CHUNK // PIECES, queries // PIECES

        def scores(t, i):
            side, j = chunks[t]
            at = j * CHUNK + i * wide
            s_buf[t % 2, :, i * wide:(i + 1) * wide] = dot(q, keys[side, :, at:at + wide])

        for i in range(PIECES):
            scores(0, i)
        for t, (side, j) in enumerate(chunks):
            ms, ls, fades = [], [], []
            for i in range(PIECES):
                if t + 1 < len(chunks):
                    scores(t + 1, i)
                at = slice(i * tall, (i + 1) * tall)
                s = s_buf[t % 2, at, :]
                top = jnp.max(s, axis=1, keepdims=True)
                m_new = top if state is None else jnp.maximum(state[0][i], top)
                p = jnp.exp2((s - m_new) * c2)
                total = jnp.sum(p, axis=1, keepdims=True)
                p_buf[at, :] = p.astype(BF16)
                if state is not None:
                    fade = jnp.exp2((state[0][i] - m_new) * c2)
                    fades.append(fade)
                    total = state[1][i] * fade + total
                ms.append(m_new)
                ls.append(total)
            o = dot_nt(p_buf[...], keys[side, :lat, j * CHUNK:(j + 1) * CHUNK])
            for i in range(PIECES):
                at = slice(i * tall, (i + 1) * tall)
                acc[at, :] = o[at] if state is None else acc[at, :] * fades[i] + o[at]
            state = (ms, ls)
        return state

    def finish(state, acc, place):
        m, l = (jnp.concatenate(x, axis=0) for x in state)
        inv = 1.0 / l
        lse = m * scale + jnp.log(l)
        lanes = lax.broadcasted_iota(jnp.int32, (seqs, vbuf.shape[-1]), 1)
        for g in range(heads):
            off, h = place(g)
            at = slice(g * seqs, (g + 1) * seqs)
            vbuf[off, h] = split_dot(acc[at, :] * inv[at], wuv_v[h])
            vbuf[off, heads] = jnp.where(lanes == h, lse[at], vbuf[off, heads])

    project_chip(0, 0)
    load_keys.wait()
    halves = tuple(tuple((side, j) for j in range(block // CHUNK)) for side in range(CORES))
    tall = heads * seqs // PIECES
    for i, (m, l) in enumerate(zip(*attend(0, None, halves[0], acc_own))):
        m_own[i * tall:(i + 1) * tall] = m
        l_own[i * tall:(i + 1) * tall] = l
    turn_queries()
    for copy in own_queries():
        copy.start()
    swap_keys().wait_recv()
    for off in near:
        for copy in arrival(off, off, mine):
            copy.wait_recv()
        for copy in relay(off):
            copy.start()
    load_wuv.wait()
    for off in near:
        for copy in arrival(chips + off, off, other):
            copy.wait_recv()
    project_near()

    def take_far(off):
        for copy in arrival(off, off, mine):
            copy.wait_recv()
        for copy in relay(off):
            copy.start()

    def near_place(lead):
        return lambda g: (near[g % 2], lead + g // 2)

    state = attend(1, None, halves[0], acc)
    if far:
        take_far(far[0])
    state = attend(1, state, halves[1], acc)
    finish(state, acc, near_place(0))
    for d in near:
        for copy in sent_part(d, 0, heads // 2, 0):
            copy.start()

    def body(unit, carry):
        off = unit

        @pl.when(unit < last)
        def _():
            for copy in arrival(chips + off, off, other):
                copy.wait_recv()
            project_chip(off, unit)
        state = attend(unit, None, halves[0] + halves[1], acc)

        @pl.when(unit + 1 < last)
        def _():
            take_far(unit + 1)

        def place(g):
            return jnp.where(unit == last, near[g % 2], off), jnp.where(unit == last, heads // 2 + g // 2, g)
        finish(state, acc, place)

        @pl.when(unit == last)
        def _():
            for d in near:
                for copy in sent_part(d, heads // 2, heads + 1, 1):
                    copy.start()

        @pl.when(unit < last)
        def _():
            for copy in sent_part(off, 0, heads + 1, 0):
                copy.start()
        return carry

    lax.fori_loop(2, units, body, 0)
    saved = tuple([ref[i * tall:(i + 1) * tall] for i in range(PIECES)] for ref in (m_own, l_own))
    state = attend(0, saved, halves[1], acc_own)
    finish(state, acc_own, lambda g: (0, g))
    for copy in own_part():
        copy.start()

    for copy in own_queries():
        copy.wait()
    for d in range(chips):
        for copy in direct(d):
            copy.wait_send()
    swap_keys().wait_send()
    for off in near + far:
        for copy in relay(off):
            copy.wait_send()
    for off in near:
        for copy in sent_part(off, 0, heads // 2, 0) + sent_part(off, heads // 2, heads + 1, 1):
            copy.wait_send()
    for off in far:
        for copy in sent_part(off, 0, heads + 1, 0):
            copy.wait_send()
    local, close = own_part()
    local.wait()
    close.wait_send()
    for off in range(chips):
        c = (chip + off) % chips
        for k, who in enumerate((par, 1 - par)):
            if off == 0 and k == 0:
                continue
            pieces = ((0, heads // 2), (heads // 2, heads + 1)) if off in near else ((0, heads + 1),)
            for turn, (lo, hi) in enumerate(pieces):
                span = pl.ds(lo, hi - lo)
                remote(vbuf.at[0, span, mine], part.at[c, who, span], p_send.at[0, 0, 0], p_recv.at[c, who, turn], partner).wait_recv()


def suffix_kernel(chips, scale, lens, q, hidden, part, w_uv, w_o, kv, out,
                  keys, q_seq, s_all, m_all, l_all, o_seq, o_all, part_v, wuv_v, wo_v, v_all, todo, ends, key_sem, w_sem):
    rows = hidden.shape[0]
    heads, lat = w_uv.shape[0], w_uv.shape[1]
    vdim = w_uv.shape[2]
    per = kv.shape[2] // SLOTS
    cut = SLOTS // LANES
    c2 = scale * LOG2E

    def each_load(b, act):
        for n in range(1, per + 1):
            @pl.when(lens[b] // SLOTS + 1 == n)
            def _():
                span = pl.ds(0, n * SLOTS)
                act(pltpu.make_async_copy(kv.at[b, :, span], keys.at[b, :, span], key_sem.at[b]))

    def plan(b, count):
        each_load(b, lambda copy: copy.start())
        for k in range(per):
            todo[count + k] = b * per + k
        count = count + lens[b] // SLOTS + 1
        ends[b // GROUP + 1] = count
        return count

    load_q = pltpu.make_async_copy(q, q_seq, w_sem.at[3])
    load_q.start()
    ends[0] = 0
    lax.fori_loop(0, rows, plan, 0)
    loads = (pltpu.make_async_copy(part, part_v, w_sem.at[0]),
             pltpu.make_async_copy(w_uv, wuv_v, w_sem.at[1]),
             pltpu.make_async_copy(w_o, wo_v, w_sem.at[2]))
    for copy in loads:
        copy.start()
    s_all[...] = jnp.full(s_all.shape, -jnp.inf, F32)
    o_seq[...] = jnp.zeros(o_seq.shape, F32)
    load_q.wait()
    lane = lax.broadcasted_iota(jnp.int32, (heads, SLOTS), 1)

    def group(g, carry):
        first, stop = ends[g], ends[g + 1]
        steps = (stop - first + UNROLL - 1) // UNROLL

        def entries(i):
            at = [first + i * UNROLL + u for u in range(UNROLL)]
            ids = [todo[jnp.minimum(a, stop - 1)] for a in at]
            return at, [(idx // per, idx % per) for idx in ids]

        def block(b, k):
            return keys[b, :, pl.ds(pl.multiple_of(k * SLOTS, SLOTS), SLOTS)]

        def score(i, carry):
            at, ids = entries(i)
            vals = [dot(q_seq[b], block(b, k)) for b, k in ids]
            for (b, k), val in zip(ids, vals):
                val = jnp.where(lane <= lens[b] - k * SLOTS, val, -jnp.inf)
                for t in range(cut):
                    s_all[k * cut + t, pl.ds(b, heads, stride=rows), :] = val[:, t * LANES:(t + 1) * LANES]
            return carry

        def gather(i, carry):
            at, ids = entries(i)
            vals = []
            for b, k in ids:
                p = jnp.concatenate([s_all[k * cut + t, pl.ds(b, heads, stride=rows), :] for t in range(cut)], axis=1)
                vals.append(dot_nt(p.astype(BF16), block(b, k)[:lat]))
            for a, (b, k), val in zip(at, ids, vals):
                o_seq[jnp.where(a < stop, b, rows)] += val
            return carry

        def arrive(b, carry):
            each_load(b, lambda copy: copy.wait())
            return carry

        lax.fori_loop(g * GROUP, (g + 1) * GROUP, arrive, 0)
        lax.fori_loop(0, steps, score, 0)
        for h in range(heads):
            at = pl.ds(pl.multiple_of(h * rows + g * GROUP, GROUP), GROUP)
            s = s_all[:, at, :]
            m = jnp.max(jnp.max(s, axis=0), axis=1, keepdims=True)
            p = jnp.exp2((s - m) * c2)
            m_all[at, :] = m
            l_all[at, :] = jnp.sum(jnp.sum(p, axis=0), axis=1, keepdims=True)
            s_all[:, at, :] = p
        lax.fori_loop(0, steps, gather, 0)
        return carry

    lax.fori_loop(0, rows // GROUP, group, 0)
    for b in range(rows):
        for t in range(lat // LANES):
            o_all[t, pl.ds(b, heads, stride=rows), :] = o_seq[b, :, t * LANES:(t + 1) * LANES]
    for copy in loads:
        copy.wait()
    half = heads // CORES
    for h in range(heads):
        at = slice(h * rows, (h + 1) * rows)
        side, i = h // half, h % half
        l = l_all[at, :]
        o = jnp.concatenate([o_all[t, at, :] for t in range(lat // LANES)], axis=1) / l
        v_suf = split_dot(o, wuv_v[h])
        lse = m_all[at, :] * scale + jnp.log(l)
        far = [part_v[c, side, half][:, i:i + 1] for c in range(chips)]
        top = functools.reduce(jnp.maximum, far, lse)
        w_suf = jnp.exp(lse - top)
        norm = w_suf
        v = v_suf * w_suf
        for c in range(chips):
            w_far = jnp.exp(far[c] - top)
            norm = norm + w_far
            v = v + part_v[c, side, i] * w_far
        v_all[:, h * vdim:(h + 1) * vdim] = (v / norm).astype(BF16)
    out[...] = (hidden[...].astype(F32) + dot(v_all[...], wo_v[...])).astype(BF16)


def solution(mesh):
    group = mesh.shape['ctx']
    chips = group // CORES
    rows_spec = P(('dp', 'ctx'), None)
    whole_spec = P()
    hbm = pl.BlockSpec(memory_space=pl.ANY)
    vmem = pl.BlockSpec(memory_space=pltpu.VMEM)
    smem = pl.BlockSpec(memory_space=pltpu.SMEM)

    def local_step(hidden, w_q, w_uk, w_uv, w_o, kv_prefix, kv_suffix, seq_lens):
        rows, dim = hidden.shape
        heads, nope, lat = w_uk.shape
        vdim = w_uv.shape[2]
        block, kv_width = kv_prefix.shape
        rot = kv_width - lat
        slots = kv_suffix.shape[1]
        scale = (w_q.shape[1] // heads) ** -0.5
        half = heads // CORES
        seqs = CORES * rows

        q_own, part = pl.pallas_call(
            functools.partial(prefix_kernel, chips, scale),
            name='prefix',
            out_shape=(jax.ShapeDtypeStruct((rows, heads, kv_width), BF16),
                       jax.ShapeDtypeStruct((chips, CORES, half + 1, rows, vdim), F32)),
            in_specs=[smem, hbm, hbm, hbm, hbm, hbm],
            out_specs=(hbm, hbm),
            scratch_shapes=[
                pltpu.VMEM((chips, seqs, dim), BF16),
                pltpu.VMEM((chips, seqs, 2 * rot), F32),
                pltpu.VMEM((pl.cdiv(kv_width, LANES), half * seqs, LANES), F32),
                pltpu.VMEM((seqs, half, kv_width), BF16),
                pltpu.VMEM((dim, w_q.shape[1] // CORES), BF16),
                pltpu.VMEM((half, nope, lat), BF16),
                pltpu.VMEM((half, lat, vdim), BF16),
                pltpu.VMEM((CORES, kv_width, block), BF16),
                pltpu.VMEM((chips, half, seqs, kv_width), BF16),
                pltpu.VMEM((half * seqs, lat), F32),
                pltpu.VMEM((half * seqs, lat), F32),
                pltpu.VMEM((half * seqs, 1), F32),
                pltpu.VMEM((half * seqs, 1), F32),
                pltpu.VMEM((2, half * seqs, CHUNK), F32),
                pltpu.VMEM((half * seqs, CHUNK), BF16),
                pltpu.VMEM((chips, half + 1, seqs, vdim), F32),
                pltpu.SemaphoreType.DMA((4,)),
                pltpu.SemaphoreType.DMA((2,)),
                pltpu.SemaphoreType.DMA((2, 2 * chips)),
                pltpu.SemaphoreType.DMA((2, 2 * chips)),
                pltpu.SemaphoreType.DMA,
                pltpu.SemaphoreType.DMA,
                pltpu.SemaphoreType.DMA((chips, 2, CORES)),
                pltpu.SemaphoreType.DMA((chips, CORES, 2)),
                pltpu.SemaphoreType.DMA((4,)),
            ],
            compiler_params=pltpu.CompilerParams(collective_id=0, has_side_effects=True, vmem_limit_bytes=VMEM_LIMIT),
        )(seq_lens, hidden, w_q, w_uk, w_uv, kv_prefix.T)

        return pl.pallas_call(
            functools.partial(suffix_kernel, chips, scale),
            name='suffix',
            out_shape=jax.ShapeDtypeStruct((rows, dim), BF16),
            in_specs=[smem, hbm, vmem, hbm, hbm, hbm, hbm],
            out_specs=vmem,
            scratch_shapes=[
                pltpu.VMEM((rows, kv_width, slots), BF16),
                pltpu.VMEM((rows, heads, kv_width), BF16),
                pltpu.VMEM((slots // LANES, heads * rows, LANES), F32),
                pltpu.VMEM((heads * rows, 1), F32),
                pltpu.VMEM((heads * rows, 1), F32),
                pltpu.VMEM((rows + 1, heads, lat), F32),
                pltpu.VMEM((lat // LANES, heads * rows, LANES), F32),
                pltpu.VMEM((chips, CORES, half + 1, rows, vdim), F32),
                pltpu.VMEM((heads, lat, vdim), BF16),
                pltpu.VMEM((heads * vdim, dim), BF16),
                pltpu.VMEM((rows, heads * vdim), BF16),
                pltpu.SMEM((rows * (slots // SLOTS) + slots // SLOTS,), jnp.int32),
                pltpu.SMEM((rows // GROUP + 1,), jnp.int32),
                pltpu.SemaphoreType.DMA((rows,)),
                pltpu.SemaphoreType.DMA((4,)),
            ],
            compiler_params=pltpu.CompilerParams(vmem_limit_bytes=67_043_328),
        )(seq_lens, q_own, hidden, part, w_uv, w_o, kv_suffix.transpose(0, 2, 1))

    return jax.shard_map(local_step, mesh=mesh, in_specs=(rows_spec, whole_spec, whole_spec, whole_spec, whole_spec, rows_spec, P(('dp', 'ctx'), None, None), P(('dp', 'ctx'))), out_specs=rows_spec, check_vma=False)
```

```python
import functools
import math
import jax
import jax.numpy as jnp
from jax import lax
from jax.experimental import pallas as pl
from jax.experimental.pallas import tpu as pltpu
from jax.sharding import PartitionSpec as P

ROPE_BASE = 10000
CORES = 2
LOG2E = math.log2(math.e)
CHUNK = 1024
PIECES = 4
SLOTS = 256
LANES = 128
UNROLL = 8
GROUP = 16
VMEM_LIMIT = 64_000_000
F32 = jnp.float32
BF16 = jnp.bfloat16
NT = (((1,), (1,)), ((), ()))


def dot(a, b):
    return jnp.dot(a, b, preferred_element_type=F32)


def dot_nt(a, b):
    return lax.dot_general(a, b, NT, preferred_element_type=F32)


def split_dot(wide, w):
    rows = wide.shape[0]
    upper = wide.astype(BF16)
    lower = (wide - upper.astype(F32)).astype(BF16)
    both = dot(jnp.concatenate([upper, lower], axis=0), w)
    return both[:rows] + both[rows:]


def rotation(lens, rows, start, rot):
    half = rot // 2
    row = lax.broadcasted_iota(jnp.int32, (rows, 2 * rot), 0)
    lane = lax.broadcasted_iota(jnp.int32, (rows, 2 * rot), 1)
    pos = jnp.zeros((rows, 2 * rot), jnp.int32)
    for b in range(rows):
        pos = jnp.where(row == b, start + lens[b], pos)
    freq = jnp.zeros((rows, 2 * rot), F32)
    for i in range(half):
        freq = jnp.where(lane % half == i, math.exp(-i * math.log(ROPE_BASE) / half), freq)
    angle = pos.astype(F32) * freq
    sin_t = jnp.sin(angle)
    return jnp.where(lane < rot, jnp.cos(angle), jnp.where(lane < rot + half, -sin_t, sin_t))


def prefix_kernel(chips, scale, lens, hidden, w_q, w_uk, w_uv, kv, q_own, part,
                  hid_all, trig_all, q_wide, q_turn, wq_v, wuk_v, wuv_v, keys, q_all, acc, acc_own, m_own, l_own, s_buf, p_buf, vbuf,
                  w_sem, key_sem, h_send, h_recv, q_send, q_recv, p_send, p_recv, own_sem):
    me = lax.axis_index('ctx')
    n = chips * CORES
    chip = me // CORES
    par = me % CORES
    rows = hidden.shape[0]
    block = kv.shape[1]
    lat = w_uk.shape[2]
    nope = w_uk.shape[1]
    heads = wuk_v.shape[0]
    rot = kv.shape[0] - lat
    width = wq_v.shape[1]
    seqs = CORES * rows
    near = (1, chips - 1)
    far = tuple(range(2, chips - 1))
    units = 2 + 1 + len(far)
    last = units - 1
    mine = pl.ds(pl.multiple_of(par * rows, rows), rows)
    other = pl.ds(pl.multiple_of((1 - par) * rows, rows), rows)
    partner = chip * CORES + (1 - par)

    def remote(src, dst, send, recv, dev):
        return pltpu.make_async_remote_copy(src_ref=src, dst_ref=dst, send_sem=send, recv_sem=recv,
                                            device_id={'ctx': dev}, device_id_type=pl.DeviceIdType.MESH)

    load_hid = pltpu.make_async_copy(hidden, hid_all.at[0, mine], own_sem.at[2])
    load_wq = pltpu.make_async_copy(w_q.at[:, pl.ds(pl.multiple_of(par * width, width), width)], wq_v, w_sem.at[0])
    load_wuk = pltpu.make_async_copy(w_uk.at[pl.ds(par * heads, heads)], wuk_v, w_sem.at[1])
    load_wuv = pltpu.make_async_copy(w_uv.at[pl.ds(par * heads, heads)], wuv_v, w_sem.at[2])
    load_keys = pltpu.make_async_copy(kv, keys.at[0], w_sem.at[3])
    load_hid.start()
    load_wq.start()
    load_wuk.start()
    load_keys.start()
    load_wuv.start()

    barrier = pltpu.get_barrier_semaphore()
    for k in range(1, n):
        pl.semaphore_signal(barrier, inc=1, device_id={'ctx': (me + k) % n}, device_id_type=pl.DeviceIdType.MESH)
    trig_all[0, mine, :] = rotation(lens, rows, n * block, rot)
    pl.semaphore_wait(barrier, n - 1)

    def both(dst, where, sems, slot, dev, src=0):
        return (remote(hid_all.at[src, mine], hid_all.at[dst, where], h_send.at[0, sems], h_recv.at[0, slot], dev),
                remote(trig_all.at[src, mine], trig_all.at[dst, where], h_send.at[1, sems], h_recv.at[1, slot], dev))

    def direct(d):
        if d == 0:
            return both(0, mine, 0, 0, partner)
        return both(chips - d, mine, d, chips - d, ((chip + d) % chips) * CORES + par)

    def relay(off):
        return both(off, mine, chips + off, chips + off, partner, src=off)

    def arrival(slot, off, where):
        return both(off, where, 0, slot, partner)

    def swap_keys():
        return remote(kv, keys.at[1], key_sem.at[0], key_sem.at[1], partner)

    load_hid.wait()
    for d in (0,) + near:
        for copy in direct(d):
            copy.start()
    swap_keys().start()
    vbuf[:, heads] = jnp.zeros((chips,) + vbuf.shape[2:], F32)
    load_wq.wait()
    load_wuk.wait()
    for copy in arrival(0, 0, other):
        copy.wait_recv()
    c2 = scale * LOG2E

    def project(hid, tri, put):
        lane = lax.broadcasted_iota(jnp.int32, (hid.shape[0], 2 * rot), 1)
        q_f = dot(hid, wq_v[...]).astype(BF16).astype(F32)
        tri_r = pltpu.roll(tri, rot, 1)
        cos_t = jnp.where(lane < rot, tri, tri_r)
        sin_t = jnp.where(lane < rot, tri_r, tri)
        for i in range(heads // 2):
            base = i * 2 * (nope + rot)
            even = q_f[:, base:base + nope]
            rest = pltpu.roll(q_f[:, base + nope:base + 2 * (nope + rot)], 2 * nope - rot, 1)
            odd = rest[:, :nope]
            pe = rest[:, nope:]
            half = rot // 2
            swapped = jnp.where(lane % rot < half, pltpu.roll(pe, 2 * rot - half, 1), pltpu.roll(pe, half, 1))
            pe = pe * cos_t + swapped * sin_t
            put(2 * i, dot(even.astype(BF16), wuk_v[2 * i]).astype(BF16), pltpu.roll(pe, rot, 1)[:, :rot].astype(BF16))
            put(2 * i + 1, dot(odd.astype(BF16), wuk_v[2 * i + 1]).astype(BF16), pe[:, :rot].astype(BF16))

    def project_chip(off, unit):
        def put(h, nope_part, rot_part):
            q_all[unit, h, :, :lat] = nope_part
            q_all[unit, h, :, lat:] = rot_part
        project(hid_all[off], trig_all[off], put)

    def project_near():
        def put(h, nope_part, rot_part):
            unit, group = (1, 2 * h) if h < heads // 2 else (last, 2 * h - heads)
            for k in range(2):
                q_all[unit, group + k, :, :lat] = nope_part[k * seqs:(k + 1) * seqs]
                q_all[unit, group + k, :, lat:] = rot_part[k * seqs:(k + 1) * seqs]
        project(jnp.concatenate([hid_all[d] for d in near], axis=0), jnp.concatenate([trig_all[d] for d in near], axis=0), put)

    def own_queries():
        to = q_own.at[:, pl.ds(pl.multiple_of(par * heads, heads), heads)]
        return (pltpu.make_async_copy(q_turn.at[mine], to, own_sem.at[0]),
                remote(q_turn.at[other], to, q_send, q_recv, partner))

    def turn_queries():
        total = lat + rot
        spans = [(t, min(LANES, total - t)) for t in range(0, total, LANES)]
        for t, w in spans:
            q_wide[t // LANES, :, :w] = q_all[0, :, :, t:t + w].reshape(heads * seqs, w).astype(F32)
        for b in range(seqs):
            for t, w in spans:
                q_turn[b, :, t:t + w] = q_wide[t // LANES, pl.ds(b, heads, stride=seqs), :][:, :w].astype(BF16)

    def own_part():
        return (pltpu.make_async_copy(vbuf.at[0, :, mine], part.at[chip, par], own_sem.at[1]),
                remote(vbuf.at[0, :, other], part.at[chip, par], p_send.at[0, 0, 1], p_recv.at[chip, par, 0], partner))

    def sent_part(off, lo, hi, turn):
        c = (chip + off) % chips
        span = pl.ds(lo, hi - lo)
        return tuple(remote(vbuf.at[off, span, where], part.at[chip, par, span], p_send.at[off, turn, k], p_recv.at[chip, par, turn], c * CORES + dev)
                     for k, (where, dev) in enumerate(((mine, par), (other, 1 - par))))

    def attend(unit, state, chunks, acc):
        queries = heads * seqs
        q = q_all[unit].reshape(queries, lat + rot)
        wide, tall = CHUNK // PIECES, queries // PIECES

        def scores(t, i):
            side, j = chunks[t]
            at = j * CHUNK + i * wide
            s_buf[t % 2, :, i * wide:(i + 1) * wide] = dot(q, keys[side, :, at:at + wide])

        for i in range(PIECES):
            scores(0, i)
        for t, (side, j) in enumerate(chunks):
            ms, ls, fades = [], [], []
            for i in range(PIECES):
                if t + 1 < len(chunks):
                    scores(t + 1, i)
                at = slice(i * tall, (i + 1) * tall)
                s = s_buf[t % 2, at, :]
                top = jnp.max(s, axis=1, keepdims=True)
                m_new = top if state is None else jnp.maximum(state[0][i], top)
                p = jnp.exp2((s - m_new) * c2)
                total = jnp.sum(p, axis=1, keepdims=True)
                p_buf[at, :] = p.astype(BF16)
                if state is not None:
                    fade = jnp.exp2((state[0][i] - m_new) * c2)
                    fades.append(fade)
                    total = state[1][i] * fade + total
                ms.append(m_new)
                ls.append(total)
            o = dot_nt(p_buf[...], keys[side, :lat, j * CHUNK:(j + 1) * CHUNK])
            for i in range(PIECES):
                at = slice(i * tall, (i + 1) * tall)
                acc[at, :] = o[at] if state is None else acc[at, :] * fades[i] + o[at]
            state = (ms, ls)
        return state

    def finish(state, acc, place):
        m, l = (jnp.concatenate(x, axis=0) for x in state)
        inv = 1.0 / l
        lse = m * scale + jnp.log(l)
        lanes = lax.broadcasted_iota(jnp.int32, (seqs, vbuf.shape[-1]), 1)
        for g in range(heads):
            off, h = place(g)
            at = slice(g * seqs, (g + 1) * seqs)
            vbuf[off, h] = split_dot(acc[at, :] * inv[at], wuv_v[h])
            vbuf[off, heads] = jnp.where(lanes == h, lse[at], vbuf[off, heads])

    project_chip(0, 0)
    for d in far:
        for copy in direct(d):
            copy.start()
    load_keys.wait()
    halves = tuple(tuple((side, j) for j in range(block // CHUNK)) for side in range(CORES))
    tall = heads * seqs // PIECES
    for i, (m, l) in enumerate(zip(*attend(0, None, halves[0], acc_own))):
        m_own[i * tall:(i + 1) * tall] = m
        l_own[i * tall:(i + 1) * tall] = l
    turn_queries()
    for copy in own_queries():
        copy.start()
    swap_keys().wait_recv()
    for off in near:
        for copy in arrival(off, off, mine):
            copy.wait_recv()
        for copy in relay(off):
            copy.start()
    load_wuv.wait()
    for off in near:
        for copy in arrival(chips + off, off, other):
            copy.wait_recv()
    project_near()

    def take_far(off):
        for copy in arrival(off, off, mine):
            copy.wait_recv()
        for copy in relay(off):
            copy.start()

    def near_place(lead):
        return lambda g: (near[g % 2], lead + g // 2)

    state = attend(1, None, halves[0], acc)
    if far:
        take_far(far[0])
    state = attend(1, state, halves[1], acc)
    finish(state, acc, near_place(0))
    for d in near:
        for copy in sent_part(d, 0, heads // 2, 0):
            copy.start()

    def body(unit, carry):
        off = unit

        @pl.when(unit < last)
        def _():
            for copy in arrival(chips + off, off, other):
                copy.wait_recv()
            project_chip(off, unit)
        state = attend(unit, None, halves[0] + halves[1], acc)

        @pl.when(unit + 1 < last)
        def _():
            take_far(unit + 1)

        def place(g):
            return jnp.where(unit == last, near[g % 2], off), jnp.where(unit == last, heads // 2 + g // 2, g)
        finish(state, acc, place)

        @pl.when(unit == last)
        def _():
            for d in near:
                for copy in sent_part(d, heads // 2, heads + 1, 1):
                    copy.start()

        @pl.when(unit < last)
        def _():
            for copy in sent_part(off, 0, heads + 1, 0):
                copy.start()
        return carry

    lax.fori_loop(2, units, body, 0)
    saved = tuple([ref[i * tall:(i + 1) * tall] for i in range(PIECES)] for ref in (m_own, l_own))
    state = attend(0, saved, halves[1], acc_own)
    finish(state, acc_own, lambda g: (0, g))
    for copy in own_part():
        copy.start()

    for copy in own_queries():
        copy.wait()
    for d in range(chips):
        for copy in direct(d):
            copy.wait_send()
    swap_keys().wait_send()
    for off in near + far:
        for copy in relay(off):
            copy.wait_send()
    for off in near:
        for copy in sent_part(off, 0, heads // 2, 0) + sent_part(off, heads // 2, heads + 1, 1):
            copy.wait_send()
    for off in far:
        for copy in sent_part(off, 0, heads + 1, 0):
            copy.wait_send()
    local, close = own_part()
    local.wait()
    close.wait_send()
    for off in range(chips):
        c = (chip + off) % chips
        for k, who in enumerate((par, 1 - par)):
            if off == 0 and k == 0:
                continue
            pieces = ((0, heads // 2), (heads // 2, heads + 1)) if off in near else ((0, heads + 1),)
            for turn, (lo, hi) in enumerate(pieces):
                span = pl.ds(lo, hi - lo)
                remote(vbuf.at[0, span, mine], part.at[c, who, span], p_send.at[0, 0, 0], p_recv.at[c, who, turn], partner).wait_recv()


def suffix_kernel(chips, scale, lens, q, hidden, part, w_uv, w_o, kv, out,
                  keys, q_seq, s_all, m_all, l_all, o_seq, o_all, part_v, wuv_v, wo_v, v_all, todo, ends, key_sem, w_sem):
    rows = hidden.shape[0]
    heads, lat = w_uv.shape[0], w_uv.shape[1]
    vdim = w_uv.shape[2]
    per = kv.shape[2] // SLOTS
    cut = SLOTS // LANES
    c2 = scale * LOG2E

    def load(idx):
        b, k = idx // per, idx % per
        span = pl.ds(pl.multiple_of(k * SLOTS, SLOTS), SLOTS)
        return pltpu.make_async_copy(kv.at[b, :, span], keys.at[idx], key_sem.at[idx])

    def plan(b, count):
        def one(k, count):
            load(b * per + k).start()
            todo[count] = b * per + k
            return count + 1
        count = lax.fori_loop(0, lens[b] // SLOTS + 1, one, count)
        ends[b // GROUP + 1] = count
        return count

    load_q = pltpu.make_async_copy(q, q_seq, w_sem.at[3])
    load_q.start()
    ends[0] = 0
    lax.fori_loop(0, rows, plan, 0)
    loads = (pltpu.make_async_copy(part, part_v, w_sem.at[0]),
             pltpu.make_async_copy(w_uv, wuv_v, w_sem.at[1]),
             pltpu.make_async_copy(w_o, wo_v, w_sem.at[2]))
    for copy in loads:
        copy.start()
    s_all[...] = jnp.full(s_all.shape, -jnp.inf, F32)
    o_seq[...] = jnp.zeros(o_seq.shape, F32)
    load_q.wait()
    lane = lax.broadcasted_iota(jnp.int32, (heads, SLOTS), 1)

    def steps(g):
        return (ends[g + 1] - ends[g] + UNROLL - 1) // UNROLL

    def entries(g, i):
        at = [ends[g] + i * UNROLL + u for u in range(UNROLL)]
        stop = ends[g + 1]
        ids = [todo[jnp.minimum(a, stop - 1)] for a in at]
        return [(idx, a < stop) for a, idx in zip(at, ids)]

    def work(scored, summed, i):
        new = entries(scored, i) if scored is not None else ()
        for idx, real in new:
            @pl.when(real)
            def _():
                load(idx).wait()
        sums = []
        for idx, real in entries(summed, i) if summed is not None else ():
            b, k = idx // per, idx % per
            p = jnp.concatenate([s_all[k * cut + t, pl.ds(b, heads, stride=rows), :] for t in range(cut)], axis=1)
            sums.append((jnp.where(real, b, rows), dot_nt(p.astype(BF16), keys[idx, :lat])))
        vals = [(idx // per, idx % per, dot(q_seq[idx // per], keys[idx])) for idx, _ in new]
        for b, k, val in vals:
            val = jnp.where(lane <= lens[b] - k * SLOTS, val, -jnp.inf)
            for t in range(cut):
                s_all[k * cut + t, pl.ds(b, heads, stride=rows), :] = val[:, t * LANES:(t + 1) * LANES]
        for to, val in sums:
            o_seq[to] += val

    def weigh(g):
        for h in range(heads):
            at = pl.ds(pl.multiple_of(h * rows + g * GROUP, GROUP), GROUP)
            s = s_all[:, at, :]
            m = jnp.max(jnp.max(s, axis=0), axis=1, keepdims=True)
            p = jnp.exp2((s - m) * c2)
            m_all[at, :] = jnp.broadcast_to(m, (GROUP, LANES))
            l_all[at, :] = jnp.broadcast_to(jnp.sum(jnp.sum(p, axis=0), axis=1, keepdims=True), (GROUP, LANES))
            s_all[:, at, :] = p

    def run(trips, scored, summed):
        def one(i, carry):
            work(scored, summed, i)
            return carry
        lax.fori_loop(0, trips, one, 0)

    groups = rows // GROUP
    run(steps(0), 0, None)
    weigh(0)

    def group(g, carry):
        run(jnp.maximum(steps(g), steps(g - 1)), g, g - 1)
        weigh(g)
        return carry

    lax.fori_loop(1, groups, group, 0)
    run(steps(groups - 1), None, groups - 1)
    for b in range(rows):
        for t in range(lat // LANES):
            o_all[t, pl.ds(b, heads, stride=rows), :] = o_seq[b, :, t * LANES:(t + 1) * LANES]
    for copy in loads:
        copy.wait()
    half = heads // CORES
    for h in range(heads):
        at = slice(h * rows, (h + 1) * rows)
        side, i = h // half, h % half
        l = l_all[at, :]
        inv = 1.0 / l
        o = jnp.concatenate([o_all[t, at, :] * inv for t in range(lat // LANES)], axis=1)
        v_suf = split_dot(o, wuv_v[h])
        lse = m_all[at, :] * scale + jnp.log(l)
        far = [jnp.broadcast_to(part_v[c, side, half][:, i:i + 1], (rows, LANES)) for c in range(chips)]
        top = functools.reduce(jnp.maximum, far, lse)
        w_suf = jnp.exp(lse - top)
        norm = w_suf
        v = v_suf * w_suf
        for c in range(chips):
            w_far = jnp.exp(far[c] - top)
            norm = norm + w_far
            v = v + part_v[c, side, i] * w_far
        v_all[:, h * vdim:(h + 1) * vdim] = (v / norm).astype(BF16)
    out[...] = (hidden[...].astype(F32) + dot(v_all[...], wo_v[...])).astype(BF16)


def solution(mesh):
    group = mesh.shape['ctx']
    chips = group // CORES
    rows_spec = P(('dp', 'ctx'), None)
    whole_spec = P()
    hbm = pl.BlockSpec(memory_space=pl.ANY)
    vmem = pl.BlockSpec(memory_space=pltpu.VMEM)
    smem = pl.BlockSpec(memory_space=pltpu.SMEM)

    def local_step(hidden, w_q, w_uk, w_uv, w_o, kv_prefix, kv_suffix, seq_lens):
        rows, dim = hidden.shape
        heads, nope, lat = w_uk.shape
        vdim = w_uv.shape[2]
        block, kv_width = kv_prefix.shape
        rot = kv_width - lat
        slots = kv_suffix.shape[1]
        scale = (w_q.shape[1] // heads) ** -0.5
        half = heads // CORES
        seqs = CORES * rows

        q_own, part = pl.pallas_call(
            functools.partial(prefix_kernel, chips, scale),
            name='prefix',
            out_shape=(jax.ShapeDtypeStruct((rows, heads, kv_width), BF16),
                       jax.ShapeDtypeStruct((chips, CORES, half + 1, rows, vdim), F32)),
            in_specs=[smem, hbm, hbm, hbm, hbm, hbm],
            out_specs=(hbm, hbm),
            scratch_shapes=[
                pltpu.VMEM((chips, seqs, dim), BF16),
                pltpu.VMEM((chips, seqs, 2 * rot), F32),
                pltpu.VMEM((pl.cdiv(kv_width, LANES), half * seqs, LANES), F32),
                pltpu.VMEM((seqs, half, kv_width), BF16),
                pltpu.VMEM((dim, w_q.shape[1] // CORES), BF16),
                pltpu.VMEM((half, nope, lat), BF16),
                pltpu.VMEM((half, lat, vdim), BF16),
                pltpu.VMEM((CORES, kv_width, block), BF16),
                pltpu.VMEM((chips, half, seqs, kv_width), BF16),
                pltpu.VMEM((half * seqs, lat), F32),
                pltpu.VMEM((half * seqs, lat), F32),
                pltpu.VMEM((half * seqs, 1), F32),
                pltpu.VMEM((half * seqs, 1), F32),
                pltpu.VMEM((2, half * seqs, CHUNK), F32),
                pltpu.VMEM((half * seqs, CHUNK), BF16),
                pltpu.VMEM((chips, half + 1, seqs, vdim), F32),
                pltpu.SemaphoreType.DMA((4,)),
                pltpu.SemaphoreType.DMA((2,)),
                pltpu.SemaphoreType.DMA((2, 2 * chips)),
                pltpu.SemaphoreType.DMA((2, 2 * chips)),
                pltpu.SemaphoreType.DMA,
                pltpu.SemaphoreType.DMA,
                pltpu.SemaphoreType.DMA((chips, 2, CORES)),
                pltpu.SemaphoreType.DMA((chips, CORES, 2)),
                pltpu.SemaphoreType.DMA((4,)),
            ],
            compiler_params=pltpu.CompilerParams(collective_id=0, has_side_effects=True, vmem_limit_bytes=VMEM_LIMIT),
        )(seq_lens, hidden, w_q, w_uk, w_uv, kv_prefix.T)

        return pl.pallas_call(
            functools.partial(suffix_kernel, chips, scale),
            name='suffix',
            out_shape=jax.ShapeDtypeStruct((rows, dim), BF16),
            in_specs=[smem, hbm, vmem, hbm, hbm, hbm, hbm],
            out_specs=vmem,
            scratch_shapes=[
                pltpu.VMEM((rows * (slots // SLOTS), kv_width, SLOTS), BF16),
                pltpu.VMEM((rows, heads, kv_width), BF16),
                pltpu.VMEM((slots // LANES, heads * rows, LANES), F32),
                pltpu.VMEM((heads * rows, LANES), F32),
                pltpu.VMEM((heads * rows, LANES), F32),
                pltpu.VMEM((rows + 1, heads, lat), F32),
                pltpu.VMEM((lat // LANES, heads * rows, LANES), F32),
                pltpu.VMEM((chips, CORES, half + 1, rows, vdim), F32),
                pltpu.VMEM((heads, lat, vdim), BF16),
                pltpu.VMEM((heads * vdim, dim), BF16),
                pltpu.VMEM((rows, heads * vdim), BF16),
                pltpu.SMEM((rows * (slots // SLOTS),), jnp.int32),
                pltpu.SMEM((rows // GROUP + 1,), jnp.int32),
                pltpu.SemaphoreType.DMA((rows * (slots // SLOTS),)),
                pltpu.SemaphoreType.DMA((4,)),
            ],
            compiler_params=pltpu.CompilerParams(vmem_limit_bytes=67_043_328),
        )(seq_lens, q_own, hidden, part, w_uv, w_o, kv_suffix.transpose(0, 2, 1))

    return jax.shard_map(local_step, mesh=mesh, in_specs=(rows_spec, whole_spec, whole_spec, whole_spec, whole_spec, rows_spec, P(('dp', 'ctx'), None, None), P(('dp', 'ctx'))), out_specs=rows_spec, check_vma=False)
```
